32 devices in a mesh: group: 2 (over y), expert: 4 (over x, core), tensor: 4 (over z).
Axes of the slice: x: 2, y: 2, z: 4, core: 2. Of those that a mesh axis runs over, the one named last changes fastest.
Arguments:
- tokens: bfloat16 [512, 4096], P(('group', 'expert'), 'tensor'), parts along dimension 0, may hold values from -6 to 6
- w_gate: bfloat16 [8, 4096, 1536], P('expert', 'tensor'), may hold values from -0.125 to 0.125
- w_up: bfloat16 [8, 4096, 1536], P('expert', 'tensor'), may hold values from -0.125 to 0.125
- w_down: bfloat16 [8, 1536, 4096], P('expert', None, 'tensor'), may hold values from -0.15625 to 0.15625
- expert_ids: int32 [512, 8], P(('group', 'expert')), parts along dimension 0, may hold values from 0 to 7, as said below
- route_weights: float32 [512, 8], P(('group', 'expert')), parts along dimension 0, may hold values from 0.05 to 0.5
Outputs:
- mixed_out: bfloat16 [512, 4096], P(('group', 'expert'), 'tensor'), parts along dimension 0
The draws below stay inside these ranges and needn't reach their ends.
There are 2 independent parts, one for each index of `group`. The reference program is written for one: setup_inputs(seed, part) draws one part's arguments, and reference() takes and returns one part's arrays. A program takes and returns all parts, laid end to end along the dimension named above; an argument that names none is the same for every part. Nothing has to cross between parts.
Inputs may be any that keep to these rules, and one draw needn't show every extreme that they name: `expert_ids`: each row names 8 different experts. In each aligned block of 64 rows no expert is named by more than 64 rows, and one expert, the same in every block of a part, is named by exactly 64 rows of every block.
All inputs are finite; a program needn't handle non-finite values.
Results may differ from the reference program's by a relative error of at most 0.0057.
Values may be sent and summed in bfloat16 or wider, within the bound.
No kernel may reach another device: no remote copies, remote signals or barrier semaphores. Data moves between devices by JAX's collectives and lax.ppermute only.
A program may use at most 128 MiB of HBM per device.

```python
import math
import jax
import jax.numpy as jnp
from jax import lax

D = 4096
FF = 1536
TOP = 8
TOK_DEV = 64
EXPERTS = 8
TOKENS = 256
BLOCKS = 4
CAP = 64


def expert_of(ordinal, hot_expert):
    return ordinal + (ordinal >= hot_expert).astype(jnp.int32)


def draw_expert_ids(key, part):
    hot_expert = jax.random.randint(jax.random.fold_in(key, 11), (), 0, EXPERTS, dtype=jnp.int32)
    pool_size = (EXPERTS - 1) * CAP
    deficit_total = EXPERTS * CAP - TOK_DEV * TOP
    block_keys = jax.random.split(jax.random.fold_in(key, 12), BLOCKS)

    def column_order(column_key):
        return jax.random.permutation(column_key, TOP).astype(jnp.int32)

    def one_block(block_key):
        sub_keys = jax.random.split(block_key, 3)
        shuffled = jax.random.permutation(sub_keys[0], pool_size).astype(jnp.int32)
        chosen = shuffled[:deficit_total] // CAP
        labels = jnp.arange(EXPERTS - 1, dtype=jnp.int32)
        deficit = jnp.sum((chosen[:, None] == labels[None, :]).astype(jnp.int32), axis=0)
        others = CAP - deficit
        counts = jnp.zeros((EXPERTS,), jnp.int32).at[expert_of(labels, hot_expert)].set(others)
        counts = counts.at[hot_expert].set(CAP)
        run_ends = jnp.cumsum(counts)
        position = jnp.arange(TOK_DEV * TOP, dtype=jnp.int32)
        sequence = jnp.sum((run_ends[None, :] <= position[:, None]).astype(jnp.int32), axis=1)
        layout = sequence.reshape(TOP, TOK_DEV).T
        row_order = jax.random.permutation(sub_keys[1], TOK_DEV).astype(jnp.int32)
        layout = layout[row_order]
        columns = jax.vmap(column_order)(jax.random.split(sub_keys[2], TOK_DEV))
        return jnp.take_along_axis(layout, columns, axis=1)
    return jax.vmap(one_block)(block_keys).reshape(TOKENS, TOP).astype(jnp.int32)


def with_spikes(entries, stream_key, source, target, shards_of, factor):
    owner, partner = [(jnp.arange(entries.shape[dim]) // (entries.shape[dim] // shards_of)).reshape([-1 if axis == dim else 1 for axis in range(entries.ndim)]) for dim in (source, target)]
    chosen = jax.random.permutation(stream_key, shards_of)[partner]
    strong = (owner == chosen) | (owner == (partner + shards_of // 2) % shards_of)
    return jnp.where(strong, factor * entries, entries)


def levels(own_key, shape, cuts, least, top_value):
    loudness, own = 1.0, jax.random.fold_in(own_key, 6)
    for dim, blocks in cuts:
        heights = jnp.exp(jax.random.uniform(jax.random.fold_in(own, dim), (blocks,), jnp.float32, least / len(cuts), top_value / len(cuts)))
        loudness = loudness * jnp.repeat(heights, shape[dim] // blocks).reshape([-1 if axis == dim else 1 for axis in range(len(shape))])
    return loudness


def scatter_about(rng, dims, width, bound, cuts=(), held_as=jnp.bfloat16):
    result = jax.random.normal(rng, dims, jnp.float32) * width
    if len(cuts) > 0:
        result = levels(rng, dims, cuts, -0.22, 0.18) * result
    return jnp.clip(result, min=-bound, max=bound).astype(held_as)


def bell_draw_with(rng, extent, deviation, bound, pieces, heavy, kind=jnp.bfloat16):
    values = deviation * jax.random.normal(rng, extent, jnp.float32)
    if pieces:
        values = values * levels(rng, extent, pieces, -0.22, 0.18)
    return jnp.clip(with_spikes(values, jax.random.fold_in(rng, 3), *heavy), -bound, bound).astype(kind)


def setup_inputs(seed: int = 0, part: int = 0) -> dict:
    keys = jax.random.split(jax.random.key(seed), 7)
    part_splits = jax.random.split(jax.random.fold_in(keys[6], part), 7)
    tokens = scatter_about(part_splits[0], (TOKENS, D), 1.0, 6.0, ((0, 4), (1, 4)))
    w_gate = bell_draw_with(keys[1], (EXPERTS, D, FF), D ** -0.5, 0.125, ((0, 4), (1, 4)), (1, 2, 4, 2.0))
    w_up = bell_draw_with(keys[2], (EXPERTS, D, FF), D ** -0.5, 0.125, ((0, 4), (1, 4)), (1, 2, 4, 2.0))
    w_down = scatter_about(keys[3], (EXPERTS, FF, D), FF ** -0.5, 0.15625, ((0, 4), (2, 4)))
    expert_ids = draw_expert_ids(jax.random.fold_in(jax.random.fold_in(keys[6], part), 71), part)
    route_weights = jnp.clip(jnp.exp(math.log(0.5) - 2.3025851 * jax.random.uniform(part_splits[5], (TOKENS, TOP), jnp.float32) ** levels(part_splits[5], (TOKENS, TOP), ((0, 4),), -0.2, 0.2)), 0.05, 0.5)
    return dict(tokens=tokens, w_gate=w_gate, w_up=w_up, w_down=w_down, expert_ids=expert_ids, route_weights=route_weights)


def slot_numbers(expert_ids):
    flat_ids = expert_ids.reshape(BLOCKS, TOK_DEV * TOP)
    labels = jnp.arange(EXPERTS, dtype=jnp.int32)
    onehot = (flat_ids[:, :, None] == labels[None, None, :]).astype(jnp.int32)
    before = jnp.cumsum(onehot, axis=1) - onehot
    return jnp.sum(before * onehot, axis=2).reshape(TOKENS, TOP).astype(jnp.int32)


def expert_block(operands):
    row_block, gate_w, up_w, down_w = operands
    gate = jnp.dot(row_block, gate_w, preferred_element_type=jnp.float32)
    up = jnp.dot(row_block, up_w, preferred_element_type=jnp.float32)
    hidden = (jax.nn.silu(gate) * up).astype(jnp.bfloat16)
    return jnp.dot(hidden, down_w, preferred_element_type=jnp.float32).astype(jnp.bfloat16)


def reference(tokens, w_gate, w_up, w_down, expert_ids, route_weights):
    slot_ids = slot_numbers(expert_ids)
    block_ids = (jnp.arange(TOKENS, dtype=jnp.int32) // TOK_DEV)[:, None] * jnp.ones((1, TOP), jnp.int32)
    position = ((expert_ids * BLOCKS + block_ids) * CAP + slot_ids).reshape(TOKENS * TOP).astype(jnp.int32)
    owners = (jnp.arange(TOKENS, dtype=jnp.int32)[:, None] * jnp.ones((1, TOP), jnp.int32)).reshape(TOKENS * TOP)
    source = jnp.full((EXPERTS * BLOCKS * CAP,), -1, jnp.int32).at[position].set(owners)
    gathered = tokens[jnp.maximum(source, 0)]
    expert_input = jnp.where((source >= 0)[:, None], gathered, jnp.zeros((), jnp.bfloat16))
    expert_input = expert_input.reshape(EXPERTS, BLOCKS * CAP, D)
    expert_output = lax.map(expert_block, (expert_input, w_gate, w_up, w_down))
    expert_output = expert_output.reshape(EXPERTS * BLOCKS * CAP, D)
    picked = expert_output[position].reshape(TOKENS, TOP, D).astype(jnp.float32)
    mixed_out = jnp.sum(picked * route_weights[:, :, None], axis=1)
    return mixed_out.astype(jnp.bfloat16)
```

```python
import jax
import jax.numpy as jnp
from jax import lax
from jax.sharding import PartitionSpec as P

CHUNKS = 4


def reduce_to_ends_and_share(gate, up, chunks):
    n = lax.axis_size("tensor")
    place = lax.axis_index("tensor")
    wire = jnp.bfloat16 if n <= 4 else jnp.float32
    experts, rows, width = gate.shape
    half = width // 2
    rb = experts * rows // chunks
    gate = gate.reshape(chunks, rb, width)
    up = up.reshape(chunks, rb, width)

    class Line:
        def __init__(self, forward):
            self.pos = place if forward else n - 1 - place
            self.cols = slice(half, width) if forward else slice(0, half)
            self.dev = (lambda p: p) if forward else (lambda p: n - 1 - p)
            self.recv = None
            self.back = None
            self.out = jnp.zeros((chunks + 1, rb, half), jnp.bfloat16)

        def own(self, k):
            g = lax.dynamic_index_in_dim(gate[:, :, self.cols], k, 0, keepdims=False)
            u = lax.dynamic_index_in_dim(up[:, :, self.cols], k, 0, keepdims=False)
            return g, u

        def send(self, t):
            if t > chunks + n - 3:
                return
            g, u = self.own(jnp.clip(t - self.pos, 0, chunks - 1))
            if self.recv is not None:
                g = g + self.recv[0].astype(jnp.float32)
                u = u + self.recv[1].astype(jnp.float32)
            pairs = [(self.dev(p), self.dev(p + 1)) for p in range(n - 1) if 0 <= t - p < chunks]
            self.recv = lax.ppermute(jnp.stack([g.astype(wire), u.astype(wire)]), "tensor", pairs)

        def finish(self, m):
            if m >= chunks:
                return None
            g = gate[m][:, self.cols] + self.recv[0].astype(jnp.float32)
            u = up[m][:, self.cols] + self.recv[1].astype(jnp.float32)
            return (jax.nn.silu(g) * u).astype(jnp.bfloat16)

        def share(self, t, mine):
            last = self.pos == n - 1
            if mine is None:
                outgoing = self.back
            else:
                self.out = self.store(jnp.where(last, t, chunks), mine)
                outgoing = mine if self.back is None else jnp.where(last, mine, self.back)
            hops = [h for h in range(n - 1) if 0 <= t - h < chunks]
            pairs = [(self.dev(n - 1 - h), self.dev(n - 2 - h)) for h in hops]
            self.back = lax.ppermute(outgoing, "tensor", pairs)
            k = t - (n - 2 - self.pos)
            ok = (k >= 0) & (k < chunks) & (self.pos < n - 1)
            self.out = self.store(jnp.where(ok, k, chunks), self.back)

        def store(self, k, block):
            return lax.dynamic_update_index_in_dim(self.out, block, k, 0)

    lines = (Line(False), Line(True))
    for t in range(chunks + 2 * n - 3):
        m = t - (n - 1)
        mine = [line.finish(m) if m >= 0 else None for line in lines]
        for line in lines:
            line.send(t)
        if m >= 0:
            for line, block in zip(lines, mine):
                line.share(m, block)
    return [line.out[:chunks].reshape(experts, rows, half) for line in lines]


def per_device(tokens, w_gate, w_up, w_down, expert_ids, route_weights):
    n_expert = lax.axis_size("expert")
    held = w_gate.shape[0]
    tok_rows, col_share = tokens.shape
    labels = jnp.arange(held * n_expert, dtype=jnp.int32)
    chosen = expert_ids[:, :, None] == labels[None, None, :]
    dense = jnp.sum(jnp.where(chosen, route_weights[:, :, None], 0.0), axis=1)
    rows_in = lax.all_gather(tokens, "expert", axis=0, tiled=True)
    dense = dense.reshape(tok_rows, n_expert, held).transpose(1, 2, 0)
    weights = lax.all_to_all(dense, "expert", split_axis=0, concat_axis=0, tiled=True)
    weights = weights.transpose(1, 0, 2).reshape(held, n_expert * tok_rows)
    gate = jnp.einsum("td,edf->etf", rows_in, w_gate, preferred_element_type=jnp.float32)
    up = jnp.einsum("td,edf->etf", rows_in, w_up, preferred_element_type=jnp.float32)
    low, high = reduce_to_ends_and_share(gate, up, CHUNKS)
    hidden = jnp.concatenate([low, high], axis=2)
    result = jnp.einsum("etf,efd->etd", hidden, w_down, preferred_element_type=jnp.float32)
    partial = jnp.sum(result * weights[:, :, None], axis=0).astype(jnp.bfloat16)
    partial = partial.reshape(n_expert, tok_rows, col_share)
    pieces = lax.all_to_all(partial, "expert", split_axis=0, concat_axis=0, tiled=True)
    return jnp.sum(pieces.astype(jnp.float32), axis=0).astype(jnp.bfloat16)


def solution(mesh):
    in_specs = (
        P(("group", "expert"), "tensor"),
        P("expert", "tensor", None),
        P("expert", "tensor", None),
        P("expert", None, "tensor"),
        P(("group", "expert"), None),
        P(("group", "expert"), None),
    )
    out_specs = P(("group", "expert"), "tensor")
    return jax.shard_map(
        per_device, mesh=mesh, in_specs=in_specs, out_specs=out_specs, check_vma=False
    )
```

```python
import jax
import jax.numpy as jnp
from jax import lax
from jax.sharding import PartitionSpec as P

SPLIT = 2


def exchange(block, bit):
    n = lax.axis_size("tensor")
    return lax.ppermute(block, "tensor", [(i, i ^ bit) for i in range(n)])


def bits_of(n):
    return [1 << j for j in range(n.bit_length() - 1)]


def reduce_step(block, bit):
    wire = jnp.bfloat16 if lax.axis_size("tensor") <= 4 else jnp.float32
    low_side = (lax.axis_index("tensor") & bit) == 0
    half = block.shape[-1] // 2
    low, high = block[..., :half], block[..., half:]
    received = exchange(jnp.where(low_side, high, low).astype(wire), bit)
    return jnp.where(low_side, low, high) + received.astype(jnp.float32)


def gather_step(block, bit):
    low_side = (lax.axis_index("tensor") & bit) == 0
    received = exchange(block, bit)
    first = jnp.where(low_side, block, received)
    second = jnp.where(low_side, received, block)
    return jnp.concatenate([first, second], axis=-1)


def activate(block):
    return (jax.nn.silu(block[0]) * block[1]).astype(jnp.bfloat16)


def per_device(tokens, w_gate, w_up, w_down, expert_ids, route_weights):
    n_expert = lax.axis_size("expert")
    held = w_gate.shape[0]
    tok_rows, col_share = tokens.shape
    labels = jnp.arange(held * n_expert, dtype=jnp.int32)
    chosen = expert_ids[:, :, None] == labels[None, None, :]
    dense = jnp.sum(jnp.where(chosen, route_weights[:, :, None], 0.0), axis=1)
    rows_in = lax.all_gather(tokens, "expert", axis=0, tiled=True)
    dense = dense.reshape(tok_rows, n_expert, held).transpose(1, 2, 0)
    weights = lax.all_to_all(dense, "expert", split_axis=0, concat_axis=0, tiled=True)
    weights = weights.transpose(1, 0, 2).reshape(held, n_expert * tok_rows)
    pieces = []
    for e in range(held):
        for r in jnp.split(rows_in, SPLIT, axis=0):
            gate = jnp.dot(r, w_gate[e], preferred_element_type=jnp.float32)
            up = jnp.dot(r, w_up[e], preferred_element_type=jnp.float32)
            pieces.append(jnp.stack([gate, up]))
    bits = bits_of(lax.axis_size("tensor"))
    steps = [lambda x, b=b: reduce_step(x, b) for b in bits]
    steps.append(activate)
    steps += [lambda x, b=b: gather_step(x, b) for b in reversed(bits)]
    for t in range(len(steps) + len(pieces) - 1):
        for m in range(len(pieces)):
            if 0 <= t - m < len(steps):
                pieces[m] = steps[t - m](pieces[m])
    partial = 0.0
    for e in range(held):
        hidden = jnp.concatenate(pieces[e * SPLIT:(e + 1) * SPLIT], axis=0)
        result = jnp.dot(hidden, w_down[e], preferred_element_type=jnp.float32)
        partial = partial + result * weights[e][:, None]
    partial = partial.astype(jnp.bfloat16)
    partial = partial.reshape(n_expert, tok_rows, col_share)
    pieces = lax.all_to_all(partial, "expert", split_axis=0, concat_axis=0, tiled=True)
    return jnp.sum(pieces.astype(jnp.float32), axis=0).astype(jnp.bfloat16)


def solution(mesh):
    in_specs = (
        P(("group", "expert"), "tensor"),
        P("expert", "tensor", None),
        P("expert", "tensor", None),
        P("expert", None, "tensor"),
        P(("group", "expert"), None),
        P(("group", "expert"), None),
    )
    out_specs = P(("group", "expert"), "tensor")
    return jax.shard_map(
        per_device, mesh=mesh, in_specs=in_specs, out_specs=out_specs, check_vma=False
    )
```

```python
import jax
import jax.numpy as jnp
from jax import lax
from jax.sharding import PartitionSpec as P

NEAR = 2


def exchange(block, bit):
    n = lax.axis_size("tensor")
    return lax.ppermute(block, "tensor", [(i, i ^ bit) for i in range(n)])


def bits_of(n):
    return [1 << j for j in range(n.bit_length() - 1)]


def reduce_step(block, bit):
    wire = jnp.bfloat16 if lax.axis_size("tensor") <= 4 else jnp.float32
    low_side = (lax.axis_index("tensor") & bit) == 0
    half = block.shape[-1] // 2
    low, high = block[..., :half], block[..., half:]
    received = exchange(jnp.where(low_side, high, low).astype(wire), bit)
    return jnp.where(low_side, low, high) + received.astype(jnp.float32)


def gather_step(block, bit):
    low_side = (lax.axis_index("tensor") & bit) == 0
    received = exchange(block, bit)
    first = jnp.where(low_side, block, received)
    second = jnp.where(low_side, received, block)
    return jnp.concatenate([first, second], axis=-1)


def activate(block):
    return (jax.nn.silu(block[0]) * block[1]).astype(jnp.bfloat16)


def meet(block, offset):
    n = lax.axis_size("expert")
    return lax.ppermute(block, "expert", [(i, i ^ offset) for i in range(n)])


def per_device(tokens, w_gate, w_up, w_down, expert_ids, route_weights):
    n_expert = lax.axis_size("expert")
    held = w_gate.shape[0]
    tok_rows, col_share = tokens.shape
    labels = jnp.arange(held * n_expert, dtype=jnp.int32)
    chosen = expert_ids[:, :, None] == labels[None, None, :]
    dense = jnp.sum(jnp.where(chosen, route_weights[:, :, None], 0.0), axis=1)
    blocks = [tokens] + [meet(tokens, d) for d in range(1, n_expert)]
    groups = [range(0, NEAR), range(NEAR, n_expert)]
    here = lax.axis_index("expert")
    bits = bits_of(lax.axis_size("tensor"))
    steps = [lambda x, b=b: reduce_step(x, b) for b in bits]
    steps.append(activate)
    steps += [lambda x, b=b: gather_step(x, b) for b in reversed(bits)]
    pieces = []
    for j, group in enumerate(groups):
        rows_in = jnp.concatenate([blocks[d] for d in group], axis=0)
        if j == 1:
            pieces[0] = steps[0](pieces[0])
            pieces[0], rows_in, dense = lax.optimization_barrier((pieces[0], rows_in, dense))
        for e in range(held):
            gate = jnp.dot(rows_in, w_gate[e], preferred_element_type=jnp.float32)
            up = jnp.dot(rows_in, w_up[e], preferred_element_type=jnp.float32)
            pieces.append(jnp.stack([gate, up]))
    dense = dense.reshape(tok_rows, n_expert, held).transpose(1, 2, 0)
    weights = lax.all_to_all(dense, "expert", split_axis=0, concat_axis=0, tiled=True)
    for t in range(len(steps) + len(pieces) - 1):
        for m in range(len(pieces)):
            if 0 <= t - m < len(steps) and t > 0:
                pieces[m] = steps[t - m](pieces[m])
    mixed = 0.0
    for j, group in enumerate(groups):
        partial = 0.0
        rows_of = jnp.concatenate([lax.dynamic_index_in_dim(weights, here ^ d, 0, False) for d in group], axis=1)
        for e in range(held):
            result = jnp.dot(pieces[j * held + e], w_down[e], preferred_element_type=jnp.float32)
            partial = partial + result * rows_of[e][:, None]
        for i, d in enumerate(group):
            block = partial[i * tok_rows:(i + 1) * tok_rows].astype(jnp.bfloat16)
            if d > 0:
                block = meet(block, d)
            mixed = mixed + block.astype(jnp.float32)
    return mixed.astype(jnp.bfloat16)


def solution(mesh):
    in_specs = (
        P(("group", "expert"), "tensor"),
        P("expert", "tensor", None),
        P("expert", "tensor", None),
        P("expert", None, "tensor"),
        P(("group", "expert"), None),
        P(("group", "expert"), None),
    )
    out_specs = P(("group", "expert"), "tensor")
    return jax.shard_map(
        per_device, mesh=mesh, in_specs=in_specs, out_specs=out_specs, check_vma=False
    )
```
